32 devices in a mesh: dp: 4 (over y, x), cls: 8 (over z, core).
Axes of the slice: x: 2, y: 2, z: 4, core: 2. Of those that a mesh axis runs over, the one named last changes fastest.
Arguments:
- embeddings: float32 [2048, 512], P('dp'), may hold values from -60 to 60, as said below
- classifier: float32 [131072, 512], P(('dp', 'cls')), may hold values from -60 to 60, as said below
- labels: int32 [2048], replicated, may hold values from 0 to 131071
- row_scale: float32 [2048], replicated, may hold values from 16 to 512
Outputs:
- loss: float32 [2048], P(('dp', 'cls'))
The draws below stay inside these ranges and needn't reach their ends.
Inputs may be any that keep to these rules, and one draw needn't show every extreme that they name: `embeddings`: rows of different scales. `classifier`: rows of different scales.
All inputs are finite; a program needn't handle non-finite values.
Results may differ from the reference program's by a relative error of at most 0.0003.
Values sent between devices are 32-bit elements; how exact they have to be, the bound alone decides.
A program may use at most 128 MiB of HBM per device.

```python
import math
import jax
import jax.numpy as jnp
from jax import lax

D = 512
CLS_DEV = 4096
EMBEDS = 2048
CLASSES = 131072


def class_row(base, index):
    row_key = jax.random.fold_in(base, index)
    return jax.random.truncated_normal(row_key, -6.0, 6.0, (D,), jnp.float32)


def many_rows(base, indices):

    def single(index):
        return class_row(base, index)
    return jax.vmap(single)(indices)


def draw_classifier(key, part):
    base = jax.random.fold_in(key, 101)
    rows = many_rows(base, jnp.arange(CLASSES, dtype=jnp.int32))
    scales = jnp.exp(jax.random.uniform(jax.random.fold_in(key, 102), (CLASSES, 1), jnp.float32, 0.0, math.log(10.0)))
    return rows * scales


def draw_embeddings(key, part):
    scales = jnp.exp(jax.random.uniform(jax.random.fold_in(key, 202), (EMBEDS, 1), jnp.float32, 0.0, math.log(10.0)))
    noise = jax.random.truncated_normal(jax.random.fold_in(key, 201), -6.0, 6.0, (EMBEDS, D), jnp.float32)
    return noise * scales


def with_ends(values, key, least, high):
    shape = values.shape
    spot = [jax.random.randint(jax.random.fold_in(key, axis), (), 0, shape[axis]) for axis in range(len(shape))]
    values = values.at[tuple(spot)].set(least)
    longest = shape.index(max(shape))
    spot[longest] = (spot[longest] + 1) % shape[longest]
    return values.at[tuple(spot)].set(high)


def setup_inputs(seed: int = 0) -> dict:
    keys = jax.random.split(jax.random.key(seed), 5)
    return {
        "embeddings": draw_embeddings(jax.random.fold_in(keys[4], 71), 0),
        "classifier": draw_classifier(jax.random.fold_in(keys[4], 71), 0),
        "labels": with_ends(jax.random.randint(keys[2], (EMBEDS,), 0, CLASSES), jax.random.fold_in(keys[2], 1), 0, CLASSES - 1).astype(jnp.int32),
        "row_scale": jnp.clip(jnp.exp(jax.random.uniform(keys[3], (EMBEDS,), jnp.float32, math.log(16.0), math.log(512.0))), 16.0, 512.0),
    }


MARGIN = 0.5
COS_MARGIN = math.cos(MARGIN)
SIN_MARGIN = math.sin(MARGIN)

def unit_rows(values):
    return values * lax.rsqrt(lax.optimization_barrier(jnp.sum(values * values, axis=-1, keepdims=True)) + 1e-06)

def margin_logit(units, picked, scales):
    cosine = lax.optimization_barrier(jnp.sum(units * picked, axis=-1))
    across = units - cosine[:, None] * picked
    sine = jnp.sqrt(lax.optimization_barrier(jnp.sum(across * across, axis=-1)))
    return scales * (cosine * COS_MARGIN - sine * SIN_MARGIN)

def block_stats(units, rows, class_ids, labels, scales, picked, owned):
    cosine = lax.dot_general(units, rows, (((1,), (1,)), ((), ())), precision=lax.Precision.HIGHEST, preferred_element_type=jnp.float32)
    target = margin_logit(units, picked, scales)
    hit = labels[:, None] == class_ids[None, :]
    logits = jnp.where(hit, target[:, None], scales[:, None] * cosine)
    peak = lax.optimization_barrier(jnp.max(logits, axis=1))
    total = lax.optimization_barrier(jnp.sum(jnp.exp(logits - peak[:, None]), axis=1))
    return (peak, total, jnp.where(owned, target, jnp.zeros_like(target)))

def merge_rows(first, second):
    peak = jnp.maximum(first[0], second[0])
    total = first[1] * jnp.exp(first[0] - peak) + second[1] * jnp.exp(second[0] - peak)
    return (peak, total, first[2] + second[2])

def reference(embeddings, classifier, labels, row_scale):
    units = unit_rows(embeddings)
    count = CLASSES // CLS_DEV
    blocks = classifier.reshape(count, CLS_DEV, D)
    numbers = jnp.arange(count).astype(jnp.int32)

    def step(carry, item):
        block, number = item
        normed = unit_rows(block)
        offset = number * CLS_DEV
        class_ids = offset + jnp.arange(CLS_DEV).astype(jnp.int32)
        owned = (labels >= offset) & (labels < offset + CLS_DEV)
        local = jnp.clip(labels - offset, 0, CLS_DEV - 1).astype(jnp.int32)
        picked = jnp.take(normed, local, axis=0)
        stats = block_stats(units, normed, class_ids, labels, row_scale, picked, owned)
        return (merge_rows(carry, stats), None)
    start = jnp.full((EMBEDS,), -1e+30, jnp.float32)
    empty = jnp.zeros((EMBEDS,), jnp.float32)
    (peak, total, target), unused = lax.scan(step, (start, empty, empty), (blocks, numbers))
    return peak + jnp.log(total) - target
```

```python
import functools
import math

import jax
import jax.numpy as jnp
from jax import lax
from jax.experimental import pallas as pl
from jax.experimental.pallas import tpu as pltpu
from jax.sharding import PartitionSpec as P

MARGIN = 0.5
COS_MARGIN = math.cos(MARGIN)
SIN_MARGIN = math.sin(MARGIN)
LOG2E = math.log2(math.e)
LN2 = math.log(2.0)
LOW = -1e30
MESH = pl.DeviceIdType.MESH


def kernel(ndp, ncls, chunk, emb_hbm, cls_hbm, lab_sm, lab_ref, scale_ref, out_ref,
           emb, raw, unit_w, picks, unit_e, inv_e, stats, got,
           emb_sem, raw_sem, xs, xr, ys, yr, ds, dr, ss, sr):
    dp, cls = lax.axis_index("dp"), lax.axis_index("cls")
    core = lax.rem(cls, 2)
    ndev = ndp * ncls
    me = dp * ncls + cls
    rows, width = cls_hbm.shape
    half = width // 2
    piece = emb_hbm.shape[0] // 4
    groups, lanes = lab_ref.shape
    nchunk = rows // chunk
    offset = me * rows

    barrier = pltpu.get_barrier_semaphore()

    @pl.loop(1, ndev)
    def _(k):
        to = lax.rem(me + k, ndev)
        pl.semaphore_signal(barrier, inc=1, device_id=(to // ncls, lax.rem(to, ncls)), device_id_type=MESH)

    emb_in = [
        pltpu.make_async_copy(emb_hbm.at[:, pl.ds(c * half, half)], emb.at[0, c], emb_sem.at[c])
        for c in range(2)
    ]
    for copy in emb_in:
        copy.start()
    raw_in = [
        pltpu.make_async_copy(raw_hbm, raw.at[pl.ds(i * chunk, chunk)], raw_sem.at[i])
        for i in range(nchunk)
        for raw_hbm in [cls_hbm.at[pl.ds(i * chunk, chunk)]]
    ]
    for copy in raw_in:
        copy.start()

    def prepare(i):
        raw_in[i].wait()

        @pl.loop(0, chunk // 256)
        def _(b):
            at = pl.ds(pl.multiple_of(i * chunk + b * 256, 256), 256)
            w = raw[at, :]
            inv = lax.rsqrt(jnp.sum(w * w, axis=1, keepdims=True) + 1e-06)
            unit_w[at, :] = (w * inv).astype(jnp.bfloat16)

    early = nchunk // 2
    for i in range(early):
        prepare(i)
    for copy in emb_in:
        copy.wait()
    pl.semaphore_wait(barrier, ndev - 1)

    to_x = (dp ^ 1, cls)
    to_y = (dp ^ 2, cls)
    partner = (dp, cls ^ 1)

    def part(slot, j):
        return emb.at[slot, core, pl.ds(j * piece, piece)]

    def send(src, dst, s, r, k, to):
        copy = pltpu.make_async_remote_copy(
            src_ref=part(*src), dst_ref=part(*dst), send_sem=s.at[k], recv_sem=r.at[k],
            device_id=to, device_id_type=MESH,
        )
        copy.start()
        return copy

    x_slot = [(1, 0), (1, 1), (1, 2), (1, 3), (3, 2), (3, 3)]
    y_slot = [(2, 2), (2, 3), (2, 0), (2, 1), (3, 0), (3, 1)]
    x_copy, y_copy, d_copy = [], [], []
    for k in range(4):
        x_copy.append(send((0, x_slot[k][1]), x_slot[k], xs, xr, k, to_x))
        y_copy.append(send((0, y_slot[k][1]), y_slot[k], ys, yr, k, to_y))
    for i in range(early, nchunk):
        prepare(i)

    def forward(k):
        x_copy[k].wait_recv()
        y_copy[k].wait_recv()
        if k < 2:
            x_copy.append(send(y_slot[k], x_slot[k + 4], xs, xr, k + 4, to_x))
            y_copy.append(send(x_slot[k], y_slot[k + 4], ys, yr, k + 4, to_y))
        d_copy.append(send(x_slot[k], x_slot[k], ds, dr, 2 * k, partner))
        d_copy.append(send(y_slot[k], y_slot[k], ds, dr, 2 * k + 1, partner))

    wide = 2 * piece
    tall = rows // 2
    group_rows = 64
    share = wide * group_rows // rows
    ids = lax.broadcasted_iota(jnp.int32, (8, wide), 0)

    def tree(parts, op):
        while len(parts) > 1:
            parts = [op(*parts[k:k + 2]) if k + 1 < len(parts) else parts[k] for k in range(0, len(parts), 2)]
        return parts[0]

    def down(row):
        return jnp.transpose(jnp.broadcast_to(row, (piece, lanes)))

    def halves(s, j):
        at = pl.ds(j * piece, piece)
        return jnp.concatenate([emb[s, 0, at, :], emb[s, 1, at, :]], axis=1)

    def quarters(values, factor):
        return [values[:, q:q + lanes] * factor for q in range(0, width, lanes)]

    def row_sum(parts):
        return jnp.sum(tree(parts, jnp.add), axis=1, keepdims=True)

    def load_unit(pair):
        for n, (s, j) in enumerate(pair):
            values = halves(s, j)
            inv = lax.rsqrt(jnp.sum(values * values, axis=1, keepdims=True) + 1e-06)
            inv_e[n * piece:(n + 1) * piece, :] = jnp.broadcast_to(inv, (piece, lanes))
            factor = down(scale_ref[pl.ds((dp ^ s) * 4 + j, 1), :] * LOG2E) * inv
            unit_e[n * piece:(n + 1) * piece, :] = jnp.concatenate(
                [v.astype(jnp.bfloat16) for v in quarters(values, factor)], axis=1)

    def sweep(pair):
        group = [(dp ^ s) * 4 + j for s, j in pair]
        local = jnp.concatenate([lab_ref[pl.ds(g, 1), :] for g in group], axis=1) - offset
        below = local - ids

        def step(i, carry):
            peak, total = carry
            logits = lax.dot_general(
                unit_w[pl.ds(pl.multiple_of(i * tall, tall), tall), :], unit_e[...], (((1,), (1,)), ((), ())),
                preferred_element_type=jnp.float32,
            )
            here = below - i * tall
            first = i * piece
            base = jnp.where(i == 0, group[0], group[1]) * piece
            for g in range(0, tall, group_rows):
                z = [jnp.where(here == r, LOW, logits[r:r + 8, :]) for r in range(g, g + group_rows, 8)]
                fresh = jnp.maximum(peak, tree(z, jnp.maximum))
                terms = [jnp.exp2(t - fresh) for t in z] + [total * jnp.exp2(peak - fresh)]
                peak, total = fresh, tree(terms, jnp.add)
                t = g // group_rows * share
                for n in range(t, t + share):
                    row = lax.rem(lab_sm[base + n], rows) if rows & (rows - 1) else lab_sm[base + n] & (rows - 1)
                    picks[pl.ds(first + n, 1), :] = raw[pl.ds(row, 1), :]
            return peak, total

        start = (jnp.full((8, wide), LOW, jnp.float32), jnp.zeros((8, wide), jnp.float32))
        peak, total = lax.fori_loop(0, 2, step, start)
        best = jnp.max(peak, axis=0, keepdims=True)
        total = jnp.sum(total * jnp.exp2(peak - best), axis=0, keepdims=True)
        for n, g in enumerate(group):
            cut = slice(n * piece, (n + 1) * piece)
            stats[pl.ds(g, 1), 0:1, :] = best[:, cut][None]
            stats[pl.ds(g, 1), 1:2, :] = total[:, cut][None]

    def finish(pair):
        for n, (s, j) in enumerate(pair):
            g = (dp ^ s) * 4 + j
            at = slice(n * piece, (n + 1) * piece)
            units = quarters(halves(s, j), inv_e[at, :])
            picked = picks[at, :]
            inv = lax.rsqrt(jnp.sum(picked * picked, axis=1, keepdims=True) + 1e-06)
            picked = quarters(picked, inv)
            cosine = row_sum([u * p for u, p in zip(units, picked)])
            across = [u - cosine * p for u, p in zip(units, picked)]
            sine = jnp.sqrt(row_sum([v * v for v in across]))
            target = cosine * COS_MARGIN - sine * SIN_MARGIN
            target = jnp.transpose(jnp.broadcast_to(target, (piece, lanes)))[0:1, :]
            local = lab_ref[pl.ds(g, 1), :] - offset
            owned = (local >= 0) & (local < rows)
            stats[pl.ds(g, 1), 2:3, :] = jnp.where(owned, scale_ref[pl.ds(g, 1), :] * target, 0.0)[None]

    pairs = [[(0, 0), (0, 1)], [(0, 2), (0, 3)]] + [[x_slot[k], y_slot[k]] for k in range(6)]

    def ready(unit):
        if 1 <= unit <= 6:
            forward(unit - 1)
        if unit >= 2:
            d_copy[2 * unit - 4].wait_recv()
            d_copy[2 * unit - 3].wait_recv()

    for unit in range(8):
        ready(unit)
        load_unit(pairs[unit])
        sweep(pairs[unit])
        finish(pairs[unit])

    share = groups * lanes // ndev
    per = lanes // share

    def outgoing(k):
        to = lax.rem(me + k, ndev)
        return pltpu.make_async_remote_copy(
            src_ref=stats.at[to // per], dst_ref=got.at[k], send_sem=ss, recv_sem=sr,
            device_id=(to // ncls, lax.rem(to, ncls)), device_id_type=MESH,
        )

    @pl.loop(1, ndev)
    def _(k):
        outgoing(k).start()

    got[0] = stats[me // per]
    for copy in x_copy + y_copy + d_copy:
        copy.wait_send()
    rest = got.at[pl.ds(1, ndev - 1)]
    pltpu.make_async_copy(rest, rest, ss).wait()
    pltpu.make_async_copy(rest, rest, sr).wait()

    everyone = got[...]
    peaks, totals = everyone[:, 0, :], everyone[:, 1, :]
    target = jnp.sum(everyone[:, 2, :], axis=0, keepdims=True)
    best = jnp.maximum(jnp.max(peaks, axis=0, keepdims=True), target * LOG2E)
    total = jnp.sum(totals * jnp.exp2(peaks - best), axis=0, keepdims=True) + jnp.exp2(target * LOG2E - best)
    loss = best * LN2 + jnp.log(total) - target
    mine = loss[:, 0:share]
    for q in range(1, per):
        mine = jnp.where(lax.rem(me, per) == q, loss[:, q * share:(q + 1) * share], mine)
    out_ref[...] = mine


def body(embeddings, classifier, labels, row_scale):
    ndp, ncls = lax.axis_size("dp"), lax.axis_size("cls")
    assert ndp == 4 and ncls % 2 == 0
    ndev = ndp * ncls
    block, width = embeddings.shape
    rows = classifier.shape[0]
    count = labels.shape[0]
    piece = block // 4
    chunk = rows // 8
    groups = count // piece
    f32 = jnp.float32
    any_spec = pl.BlockSpec(memory_space=pl.ANY)
    vmem = pl.BlockSpec(memory_space=pltpu.VMEM)
    dma = pltpu.SemaphoreType.DMA
    out = pl.pallas_call(
        functools.partial(kernel, ndp, ncls, chunk),
        out_shape=jax.ShapeDtypeStruct((1, count // ndev), f32),
        in_specs=[any_spec, any_spec, pl.BlockSpec(memory_space=pltpu.SMEM), vmem, vmem],
        out_specs=vmem,
        scratch_shapes=[
            pltpu.VMEM((4, 2, block, width // 2), f32),
            pltpu.VMEM((rows, width), f32),
            pltpu.VMEM((rows, width), jnp.bfloat16),
            pltpu.VMEM((2 * piece, width), f32),
            pltpu.VMEM((2 * piece, width), jnp.bfloat16),
            pltpu.VMEM((2 * piece, 128), f32),
            pltpu.VMEM((groups, 8, piece), f32),
            pltpu.VMEM((ndev, 8, piece), f32),
            dma((2,)), dma((8,)), dma((6,)), dma((6,)), dma((6,)), dma((6,)),
            dma((12,)), dma((12,)), dma, dma,
        ],
        compiler_params=pltpu.CompilerParams(
            collective_id=0, has_side_effects=True, vmem_limit_bytes=56 * 1024 * 1024
        ),
    )(embeddings, classifier, labels, labels.reshape(groups, piece), row_scale.reshape(groups, piece))
    return out.reshape(count // ndev)


def solution(mesh):
    placed = (P("dp", None), P(("dp", "cls"), None), P(), P())
    return jax.shard_map(
        body, mesh=mesh, in_specs=placed, out_specs=P(("dp", "cls")), check_vma=False
    )
```

```python
import functools
import math

import jax
import jax.numpy as jnp
from jax import lax
from jax.experimental import pallas as pl
from jax.experimental.pallas import tpu as pltpu
from jax.sharding import PartitionSpec as P

MARGIN = 0.5
COS_MARGIN = math.cos(MARGIN)
SIN_MARGIN = math.sin(MARGIN)
LOG2E = math.log2(math.e)
LN2 = math.log(2.0)
LOW = -1e30
MESH = pl.DeviceIdType.MESH
F, N = 0, 1


def tree(parts, op):
    while len(parts) > 1:
        parts = [op(*parts[k:k + 2]) if k + 1 < len(parts) else parts[k] for k in range(0, len(parts), 2)]
    return parts[0]


def kernel(ndp, ncls, chunk, emb_hbm, cls_hbm, lab_sm, lab_ref, scale_ref, out_ref,
           emb, raw, unit_w, picks, unit_e, inv_e, stats, got,
           emb_sem, raw_sem, xs, xr, ys, yr, zs, zr, ds, dr, ss, sr):
    dp, cls = lax.axis_index("dp"), lax.axis_index("cls")
    core = lax.rem(cls, 2)
    ndev = ndp * ncls
    me = dp * ncls + cls
    rows, width = cls_hbm.shape
    piece = emb_hbm.shape[0] // 8
    part = piece // 2
    groups, lanes = lab_ref.shape
    nchunk = rows // chunk
    offset = me * rows
    share = groups * lanes // ndev

    emb_in = pltpu.make_async_copy(emb_hbm, emb.at[0], emb_sem)
    emb_in.start()
    barrier = pltpu.get_barrier_semaphore()

    @pl.loop(1, ndev)
    def _(k):
        to = lax.rem(me + k, ndev)
        pl.semaphore_signal(barrier, inc=1, device_id=(to // ncls, lax.rem(to, ncls)), device_id_type=MESH)

    raw_in = [
        pltpu.make_async_copy(cls_hbm.at[pl.ds(i * chunk, chunk)], raw.at[pl.ds(i * chunk, chunk)], raw_sem.at[i])
        for i in range(nchunk)
    ]
    for copy in raw_in:
        copy.start()
    emb_in.wait()
    pl.semaphore_wait(barrier, ndev - 1)

    to_x = (dp ^ 1, cls)
    to_y = (dp ^ 2, cls)
    to_z = (dp, cls ^ 2)
    partner = (dp, cls ^ 1)
    near = cls * share // (4 * piece) * 4
    starts = (4 - near, near)
    turn = lax.rem(cls // 2, 2) * 2
    sx = (0, turn)
    sy = (2, -turn)

    def place(half, index):
        base, shift = index
        return starts[half] + base + shift

    def at(index, by):
        return (index[0] + by, index[1])

    def own(slot, p):
        return emb.at[slot, pl.ds(p * piece + core * part, part)]

    def send(source, slot, p, s, r, k, to):
        copy = pltpu.make_async_remote_copy(
            src_ref=own(source, p), dst_ref=own(slot, p), send_sem=s.at[k], recv_sem=r.at[k],
            device_id=to, device_id_type=MESH,
        )
        copy.start()
        return copy

    x_plan = [(1, F, sx), (1, F, at(sx, 1)), (1, N, sx), (1, N, at(sx, 1)), (3, F, sy), (3, F, at(sy, 1)),
              (1, N, at(sy, 1)), (3, N, sy), (3, N, at(sy, 1))]
    y_plan = [(2, F, at(sy, 1)), (2, F, sy), (2, N, at(sy, 1)), (2, N, sy), (3, F, at(sx, 1)), (3, F, sx),
              (2, N, sx), (3, N, at(sx, 1)), (3, N, sx)]
    z_plan = [(1, F, sx), (2, F, at(sy, 1)), (1, F, at(sx, 1)), (2, F, sy), (1, N, sx), (2, N, at(sy, 1))]

    def other(index):
        return (2 - index[0] if index[0] % 2 == 0 else 4 - index[0], -index[1])

    came_z = [(slot, half, other(index)) for slot, half, index in z_plan]

    def remote(spot, source, s, r, k, to):
        slot, half, index = spot
        p = place(half, index)
        return pltpu.make_async_remote_copy(
            src_ref=own(source, p), dst_ref=own(slot, p), send_sem=s.at[k], recv_sem=r.at[k],
            device_id=to, device_id_type=MESH,
        )

    def x_copy(k):
        return remote(x_plan[k], 0 if x_plan[k][0] == 1 else 2, xs, xr, k, to_x)

    def y_copy(k):
        return remote(y_plan[k], 0 if y_plan[k][0] == 2 else 1, ys, yr, k, to_y)

    def z_copy(k):
        return remote(z_plan[k], z_plan[k][0], zs, zr, k, to_z)

    def d_copy(k):
        copy, plan, n = d_order[k]
        return remote(plan[n], plan[n][0], ds, dr, k, partner)

    X, Y, Z = (x_copy, x_plan), (y_copy, y_plan), (z_copy, came_z)
    arrivals = [
        [(*X, 0), (*Y, 0)],
        [(*X, 1), (*Y, 1)],
        [(*X, 2), (*Y, 2), (*X, 3), (*Y, 3)],
        [(*Z, 0), (*Z, 1), (*X, 4), (*Y, 4)],
        [(*Z, 2), (*X, 5), (*Y, 5), (*Z, 3)],
        [(*X, 6), (*Y, 6), (*Z, 4), (*Z, 5)],
        [(*X, 7), (*Y, 7), (*X, 8), (*Y, 8)],
    ]
    relays = [
        [(z_copy, 0), (z_copy, 1)],
        [(x_copy, 4), (y_copy, 4), (z_copy, 2), (z_copy, 3), (x_copy, 5), (y_copy, 5), (x_copy, 6), (y_copy, 6)],
        [(z_copy, 4), (z_copy, 5), (x_copy, 7), (y_copy, 7), (x_copy, 8), (y_copy, 8)],
        [], [], [], [],
    ]
    d_order = [entry for step in arrivals for entry in step]

    def forward(step):
        done = sum(len(group) for group in arrivals[:step])
        for n, (copy, _, k) in enumerate(arrivals[step]):
            copy(k).wait_recv()
            d_copy(done + n).start()
        for copy, k in relays[step]:
            copy(k).start()

    for k in range(4):
        x_copy(k).start()
        y_copy(k).start()

    def prepare(i):
        raw_in[i].wait()

        @pl.loop(0, chunk // 256)
        def _(b):
            rows_at = pl.ds(pl.multiple_of(i * chunk + b * 256, 256), 256)
            w = raw[rows_at, :]
            inv = lax.rsqrt(jnp.sum(w * w, axis=1, keepdims=True) + 1e-06)
            unit_w[rows_at, :] = (w * inv).astype(jnp.bfloat16)

    for i in range(nchunk):
        prepare(i)

    zx, zy = sy, sx
    units = [
        [(0, F, (0, 0)), (0, F, (1, 0)), (0, F, (2, 0)), (0, F, (3, 0))],
        [(0, N, (0, 0)), (0, N, (1, 0)), (0, N, (2, 0)), (0, N, (3, 0))],
        [(1, F, sx), (1, F, at(sx, 1)), (2, F, sy), (2, F, at(sy, 1))],
        [(1, N, sx), (1, N, at(sx, 1)), (2, N, sy), (2, N, at(sy, 1))],
        [(1, F, zx), (2, F, at(zy, 1)), (3, F, sy), (3, F, at(sx, 1))],
        [(3, F, sx), (3, F, at(sy, 1)), (2, F, zy), (1, F, at(zx, 1))],
        [(2, N, sx), (1, N, at(sy, 1)), (1, N, zx), (2, N, at(zy, 1))],
        [(3, N, sy), (3, N, at(sy, 1)), (3, N, sx), (3, N, at(sx, 1))],
    ]
    wide = 4 * piece
    tall = rows // 2
    group_rows = 64
    ids = lax.broadcasted_iota(jnp.int32, (8, wide), 0)
    first_half = lax.broadcasted_iota(jnp.int32, (1, lanes), 1) < piece

    def where_of(spot):
        slot, half, index = spot
        return slot, dp ^ slot, place(half, index)

    def row_of(ref, pair):
        both = []
        for spot in pair:
            _, block, p = where_of(spot)
            both.append(ref[pl.ds(block * 4 + p // 2, 1), :])
        return jnp.where(first_half, both[0], both[1])

    def values_of(pair):
        both = []
        for spot in pair:
            slot, _, p = where_of(spot)
            both.append(emb[slot, pl.ds(pl.multiple_of(p * piece, piece), piece), :])
        return jnp.concatenate(both, axis=0)

    def quarters(values, factor):
        return [values[:, q:q + lanes] * factor for q in range(0, width, lanes)]

    def row_sum(parts):
        return jnp.sum(tree(parts, jnp.add), axis=1, keepdims=True)

    def flip(values):
        return jnp.transpose(jnp.broadcast_to(values, (lanes, lanes)))

    def load_unit(unit):
        for n in range(2):
            pair = unit[2 * n:2 * n + 2]
            values = values_of(pair)
            inv = lax.rsqrt(jnp.sum(values * values, axis=1, keepdims=True) + 1e-06)
            rows_at = slice(n * lanes, (n + 1) * lanes)
            inv_e[rows_at, :] = jnp.broadcast_to(inv, (lanes, lanes))
            factor = flip(row_of(scale_ref, pair) * LOG2E) * inv
            unit_e[rows_at, :] = jnp.concatenate(
                [v.astype(jnp.bfloat16) for v in quarters(values, factor)], axis=1)

    def sweep(unit, below, hook):
        bases = []
        for spot in unit:
            _, block, p = where_of(spot)
            bases.append((block * 8 + p) * piece)
        count = lanes * group_rows // tall

        def step(i, carry):
            peak, total = carry
            logits = lax.dot_general(
                unit_w[pl.ds(pl.multiple_of(i * tall, tall), tall), :], unit_e[...], (((1,), (1,)), ((), ())),
                preferred_element_type=jnp.float32,
            )
            here = below - i * tall
            base = [jnp.where(i == 0, bases[k], bases[2 + k]) for k in range(2)]
            for g in range(0, tall, group_rows):
                z = [jnp.where(here == r, LOW, logits[r:r + 8, :]) for r in range(g, g + group_rows, 8)]
                fresh = jnp.maximum(peak, tree(z, jnp.maximum))
                terms = [jnp.exp2(t - fresh) for t in z] + [total * jnp.exp2(peak - fresh)]
                peak, total = fresh, tree(terms, jnp.add)
                t = g // group_rows * count
                for n in range(t, t + count):
                    label = lab_sm[base[n // piece] + n % piece]
                    row = lax.rem(label, rows) if rows & (rows - 1) else label & (rows - 1)
                    picks[pl.ds(i * lanes + n, 1), :] = raw[pl.ds(row, 1), :]
            if hook is not None:
                pl.when(i == 0)(lambda: forward(hook))
            return peak, total

        start = (jnp.full((8, wide), LOW, jnp.float32), jnp.zeros((8, wide), jnp.float32))
        return lax.fori_loop(0, 2, step, start)

    def finish(number, unit, local, peak, total):
        best = jnp.max(peak, axis=0, keepdims=True)
        total = jnp.sum(total * jnp.exp2(peak - best), axis=0, keepdims=True)
        for n in range(2):
            pair = unit[2 * n:2 * n + 2]
            rows_at = slice(n * lanes, (n + 1) * lanes)
            embs = quarters(values_of(pair), inv_e[rows_at, :])
            picked = picks[rows_at, :]
            inv = lax.rsqrt(jnp.sum(picked * picked, axis=1, keepdims=True) + 1e-06)
            picked = quarters(picked, inv)
            cosine = row_sum([u * p for u, p in zip(embs, picked)])
            across = [u - cosine * p for u, p in zip(embs, picked)]
            sine = jnp.sqrt(row_sum([v * v for v in across]))
            target = flip(cosine * COS_MARGIN - sine * SIN_MARGIN)[0:1, :]
            mine = local[:, rows_at]
            owned = (mine >= 0) & (mine < rows)
            tile = 2 * number + n
            stats[tile, 0:1, :] = best[:, rows_at]
            stats[tile, 1:2, :] = total[:, rows_at]
            stats[tile, 2:3, :] = jnp.where(owned, row_of(scale_ref, pair) * target, 0.0)

    def report(number, unit):
        for n, spot in enumerate(unit):
            _, block, p = where_of(spot)

            @pl.loop(0, piece // share)
            def _(t, tile=2 * number + n // 2, start=block * ncls + p * (piece // share)):
                to = start + t

                @pl.when(to != me)
                def _():
                    pltpu.make_async_remote_copy(
                        src_ref=stats.at[tile], dst_ref=got.at[me], send_sem=ss, recv_sem=sr,
                        device_id=(to // ncls, lax.rem(to, ncls)), device_id_type=MESH,
                    ).start()

    stats[:, 3:4, :] = jnp.zeros((2 * len(units), 1, lanes), jnp.float32)
    arrived = 0
    for number, unit in enumerate(units):
        while number >= 2 and arrived < 4 * (number - 1):
            d_copy(arrived).wait_recv()
            arrived += 1
        load_unit(unit)
        local = jnp.concatenate([row_of(lab_ref, unit[0:2]), row_of(lab_ref, unit[2:4])], axis=1) - offset
        below = local - ids
        carry = sweep(unit, below, number if 1 <= number <= 6 else None)
        if number == 0:
            forward(0)
        finish(number, unit, local, *carry)
        report(number, unit)

    got[me] = stats[2 + lax.rem(cls * share // piece, 4) // 2]
    for copy, plan in ((x_copy, x_plan), (y_copy, y_plan), (z_copy, z_plan), (d_copy, d_order)):
        for k in range(len(plan)):
            copy(k).wait_send()
    rest = got.at[pl.ds(0, ndev - 1)]
    pltpu.make_async_copy(rest, rest, ss).wait()
    pltpu.make_async_copy(rest, rest, sr).wait()

    peaks, totals = got[:, 0, :], got[:, 1, :]
    target = jnp.sum(got[:, 2, :], axis=0, keepdims=True)
    best = jnp.maximum(jnp.max(peaks, axis=0, keepdims=True), target * LOG2E)
    total = jnp.sum(totals * jnp.exp2(peaks - best), axis=0, keepdims=True) + jnp.exp2(target * LOG2E - best)
    loss = best * LN2 + jnp.log(total) - target
    per = lanes // share
    mine = loss[:, 0:share]
    for q in range(1, per):
        mine = jnp.where(lax.rem(me, per) == q, loss[:, q * share:(q + 1) * share], mine)
    out_ref[...] = mine


def body(embeddings, classifier, labels, row_scale):
    ndp, ncls = lax.axis_size("dp"), lax.axis_size("cls")
    assert ndp == 4 and ncls % 4 == 0
    ndev = ndp * ncls
    block, width = embeddings.shape
    rows = classifier.shape[0]
    count = labels.shape[0]
    lanes = block // 4
    chunk = rows // 8
    groups = count // lanes
    f32 = jnp.float32
    any_spec = pl.BlockSpec(memory_space=pl.ANY)
    vmem = pl.BlockSpec(memory_space=pltpu.VMEM)
    dma = pltpu.SemaphoreType.DMA
    out = pl.pallas_call(
        functools.partial(kernel, ndp, ncls, chunk),
        out_shape=jax.ShapeDtypeStruct((1, count // ndev), f32),
        in_specs=[any_spec, any_spec, pl.BlockSpec(memory_space=pltpu.SMEM), vmem, vmem],
        out_specs=vmem,
        scratch_shapes=[
            pltpu.VMEM((4, block, width), f32),
            pltpu.VMEM((rows, width), f32),
            pltpu.VMEM((rows, width), jnp.bfloat16),
            pltpu.VMEM((2 * lanes, width), f32),
            pltpu.VMEM((2 * lanes, width), jnp.bfloat16),
            pltpu.VMEM((2 * lanes, lanes), f32),
            pltpu.VMEM((16, 4, lanes), f32),
            pltpu.VMEM((ndev, 4, lanes), f32),
            dma, dma((8,)), dma((9,)), dma((9,)), dma((9,)), dma((9,)), dma((6,)), dma((6,)),
            dma((24,)), dma((24,)), dma, dma,
        ],
        compiler_params=pltpu.CompilerParams(
            collective_id=0, has_side_effects=True, vmem_limit_bytes=56 * 1024 * 1024
        ),
    )(embeddings, classifier, labels, labels.reshape(groups, lanes), row_scale.reshape(groups, lanes))
    return out.reshape(count // ndev)


def solution(mesh):
    placed = (P("dp", None), P(("dp", "cls"), None), P(), P())
    return jax.shard_map(
        body, mesh=mesh, in_specs=placed, out_specs=P(("dp", "cls")), check_vma=False
    )
```

```python
import functools
import math

import jax
import jax.numpy as jnp
from jax import lax
from jax.experimental import pallas as pl
from jax.experimental.pallas import tpu as pltpu
from jax.sharding import PartitionSpec as P

MARGIN = 0.5
COS_MARGIN = math.cos(MARGIN)
SIN_MARGIN = math.sin(MARGIN)
LOG2E = math.log2(math.e)
LN2 = math.log(2.0)
LOW = -1e30
MESH = pl.DeviceIdType.MESH
F, N = 0, 1


def tree(parts, op):
    while len(parts) > 1:
        parts = [op(*parts[k:k + 2]) if k + 1 < len(parts) else parts[k] for k in range(0, len(parts), 2)]
    return parts[0]


def kernel(ndp, ncls, chunk, emb_hbm, cls_hbm, lab_sm, lab_ref, scale_ref, out_ref,
           emb, raw, unit_w, picks, unit_e, inv_e, stats, got,
           emb_sem, raw_sem, xs, xr, ys, yr, zs, zr, ds, dr, ss, sr, rounds):
    dp, cls = lax.axis_index("dp"), lax.axis_index("cls")
    core = lax.rem(cls, 2)
    ndev = ndp * ncls
    me = dp * ncls + cls
    rows, width = cls_hbm.shape
    piece = emb_hbm.shape[0] // 8
    part = piece // 2
    groups, lanes = lab_ref.shape
    nchunk = rows // chunk
    offset = me * rows
    share = groups * lanes // ndev

    emb_in = pltpu.make_async_copy(emb_hbm, emb.at[0], emb_sem)
    emb_in.start()
    to_x = (dp ^ 1, cls)
    to_y = (dp ^ 2, cls)
    to_z = (dp, cls ^ 2)
    partner = (dp, cls ^ 1)
    has_low, has_high = cls >= 2, cls + 2 < ncls
    beside = 3 + has_low.astype(jnp.int32) + has_high.astype(jnp.int32)

    def greet(sem):
        for to in (to_x, to_y, partner):
            pl.semaphore_signal(sem, inc=1, device_id=to, device_id_type=MESH)

        @pl.when(has_low)
        def _():
            pl.semaphore_signal(sem, inc=1, device_id=(dp, cls - 2), device_id_type=MESH)

        @pl.when(has_high)
        def _():
            pl.semaphore_signal(sem, inc=1, device_id=(dp, cls + 2), device_id_type=MESH)

    barrier = pltpu.get_barrier_semaphore()
    greet(barrier)

    raw_in = [
        pltpu.make_async_copy(cls_hbm.at[pl.ds(i * chunk, chunk)], raw.at[pl.ds(i * chunk, chunk)], raw_sem.at[i])
        for i in range(nchunk)
    ]
    for copy in raw_in:
        copy.start()
    emb_in.wait()
    pl.semaphore_wait(barrier, beside)
    last_round = ncls // 2
    greet(rounds.at[0])

    def hear(r):
        pl.semaphore_wait(rounds.at[r], beside)
        if r < last_round:
            greet(rounds.at[r + 1])

    near = cls * share // (4 * piece) * 4
    starts = (4 - near, near)
    turn = lax.rem(cls // 2, 2) * 2
    sx = (0, turn)
    sy = (2, -turn)

    def place(half, index):
        base, shift = index
        return starts[half] + base + shift

    def at(index, by):
        return (index[0] + by, index[1])

    def own(slot, p):
        return emb.at[slot, pl.ds(p * piece + core * part, part)]

    def send(source, slot, p, s, r, k, to):
        copy = pltpu.make_async_remote_copy(
            src_ref=own(source, p), dst_ref=own(slot, p), send_sem=s.at[k], recv_sem=r.at[k],
            device_id=to, device_id_type=MESH,
        )
        copy.start()
        return copy

    x_plan = [(1, F, sx), (1, F, at(sx, 1)), (1, N, sx), (1, N, at(sx, 1)), (3, F, sy), (3, F, at(sy, 1)),
              (1, N, at(sy, 1)), (3, N, sy), (3, N, at(sy, 1))]
    y_plan = [(2, F, at(sy, 1)), (2, F, sy), (2, N, at(sy, 1)), (2, N, sy), (3, F, at(sx, 1)), (3, F, sx),
              (2, N, sx), (3, N, at(sx, 1)), (3, N, sx)]
    z_plan = [(1, F, sx), (2, F, at(sy, 1)), (1, F, at(sx, 1)), (2, F, sy), (1, N, sx), (2, N, at(sy, 1))]

    def other(index):
        return (2 - index[0] if index[0] % 2 == 0 else 4 - index[0], -index[1])

    came_z = [(slot, half, other(index)) for slot, half, index in z_plan]

    def remote(spot, source, s, r, k, to):
        slot, half, index = spot
        p = place(half, index)
        return pltpu.make_async_remote_copy(
            src_ref=own(source, p), dst_ref=own(slot, p), send_sem=s.at[k], recv_sem=r.at[k],
            device_id=to, device_id_type=MESH,
        )

    def x_copy(k):
        return remote(x_plan[k], 0 if x_plan[k][0] == 1 else 2, xs, xr, k, to_x)

    def y_copy(k):
        return remote(y_plan[k], 0 if y_plan[k][0] == 2 else 1, ys, yr, k, to_y)

    def z_copy(k):
        return remote(z_plan[k], z_plan[k][0], zs, zr, k, to_z)

    def d_copy(k):
        copy, plan, n = d_order[k]
        return remote(plan[n], plan[n][0], ds, dr, k, partner)

    X, Y, Z = (x_copy, x_plan), (y_copy, y_plan), (z_copy, came_z)
    arrivals = [
        [(*X, 0), (*Y, 0)],
        [(*X, 1), (*Y, 1)],
        [(*X, 2), (*Y, 2), (*X, 3), (*Y, 3)],
        [(*Z, 0), (*Z, 1), (*X, 4), (*Y, 4)],
        [(*Z, 2), (*X, 5), (*Y, 5), (*Z, 3)],
        [(*X, 6), (*Y, 6), (*Z, 4), (*Z, 5)],
        [(*X, 7), (*Y, 7), (*X, 8), (*Y, 8)],
    ]
    relays = [
        [(z_copy, 0), (z_copy, 1)],
        [(x_copy, 4), (y_copy, 4), (z_copy, 2), (z_copy, 3), (x_copy, 5), (y_copy, 5), (x_copy, 6), (y_copy, 6)],
        [(z_copy, 4), (z_copy, 5), (x_copy, 7), (y_copy, 7), (x_copy, 8), (y_copy, 8)],
        [], [], [], [],
    ]
    d_order = [entry for step in arrivals for entry in step]

    def forward(step):
        done = sum(len(group) for group in arrivals[:step])
        for n, (copy, _, k) in enumerate(arrivals[step]):
            copy(k).wait_recv()
            d_copy(done + n).start()
        for copy, k in relays[step]:
            copy(k).start()

    for k in range(4):
        x_copy(k).start()
        y_copy(k).start()

    def prepare(i):
        raw_in[i].wait()

        @pl.loop(0, chunk // 256)
        def _(b):
            rows_at = pl.ds(pl.multiple_of(i * chunk + b * 256, 256), 256)
            w = raw[rows_at, :]
            inv = lax.rsqrt(jnp.sum(w * w, axis=1, keepdims=True) + 1e-06)
            unit_w[rows_at, :] = (w * inv).astype(jnp.bfloat16)

    for i in range(nchunk):
        prepare(i)
    hear(0)

    zx, zy = sy, sx
    units = [
        [(0, F, (0, 0)), (0, F, (1, 0)), (0, F, (2, 0)), (0, F, (3, 0))],
        [(0, N, (0, 0)), (0, N, (1, 0)), (0, N, (2, 0)), (0, N, (3, 0))],
        [(1, F, sx), (1, F, at(sx, 1)), (2, F, sy), (2, F, at(sy, 1))],
        [(1, N, sx), (1, N, at(sx, 1)), (2, N, sy), (2, N, at(sy, 1))],
        [(1, F, zx), (2, F, at(zy, 1)), (3, F, sy), (3, F, at(sx, 1))],
        [(3, F, sx), (3, F, at(sy, 1)), (2, F, zy), (1, F, at(zx, 1))],
        [(2, N, sx), (1, N, at(sy, 1)), (1, N, zx), (2, N, at(zy, 1))],
        [(3, N, sy), (3, N, at(sy, 1)), (3, N, sx), (3, N, at(sx, 1))],
    ]
    wide = 4 * piece
    tall = rows // 2
    group_rows = 64
    ids = lax.broadcasted_iota(jnp.int32, (8, wide), 0)
    first_half = lax.broadcasted_iota(jnp.int32, (1, lanes), 1) < piece

    def where_of(spot):
        slot, half, index = spot
        return slot, dp ^ slot, place(half, index)

    def row_of(ref, pair):
        both = []
        for spot in pair:
            _, block, p = where_of(spot)
            both.append(ref[pl.ds(block * 4 + p // 2, 1), :])
        return jnp.where(first_half, both[0], both[1])

    def values_of(pair):
        both = []
        for spot in pair:
            slot, _, p = where_of(spot)
            both.append(emb[slot, pl.ds(pl.multiple_of(p * piece, piece), piece), :])
        return jnp.concatenate(both, axis=0)

    def quarters(values, factor):
        return [values[:, q:q + lanes] * factor for q in range(0, width, lanes)]

    def row_sum(parts):
        return jnp.sum(tree(parts, jnp.add), axis=1, keepdims=True)

    def flip(values):
        return jnp.transpose(jnp.broadcast_to(values, (lanes, lanes)))

    def load_unit(unit):
        for n in range(2):
            pair = unit[2 * n:2 * n + 2]
            values = values_of(pair)
            inv = lax.rsqrt(jnp.sum(values * values, axis=1, keepdims=True) + 1e-06)
            rows_at = slice(n * lanes, (n + 1) * lanes)
            inv_e[rows_at, :] = jnp.broadcast_to(inv, (lanes, lanes))
            factor = flip(row_of(scale_ref, pair) * LOG2E) * inv
            unit_e[rows_at, :] = jnp.concatenate(
                [v.astype(jnp.bfloat16) for v in quarters(values, factor)], axis=1)

    def sweep(unit, below, hook):
        bases = []
        for spot in unit:
            _, block, p = where_of(spot)
            bases.append((block * 8 + p) * piece)
        count = lanes * group_rows // tall

        def step(i, carry):
            peak, total = carry
            logits = lax.dot_general(
                unit_w[pl.ds(pl.multiple_of(i * tall, tall), tall), :], unit_e[...], (((1,), (1,)), ((), ())),
                preferred_element_type=jnp.float32,
            )
            here = below - i * tall
            base = [jnp.where(i == 0, bases[k], bases[2 + k]) for k in range(2)]
            for g in range(0, tall, group_rows):
                z = [jnp.where(here == r, LOW, logits[r:r + 8, :]) for r in range(g, g + group_rows, 8)]
                fresh = jnp.maximum(peak, tree(z, jnp.maximum))
                terms = [jnp.exp2(t - fresh) for t in z] + [total * jnp.exp2(peak - fresh)]
                peak, total = fresh, tree(terms, jnp.add)
                t = g // group_rows * count
                for n in range(t, t + count):
                    label = lab_sm[base[n // piece] + n % piece]
                    row = lax.rem(label, rows) if rows & (rows - 1) else label & (rows - 1)
                    picks[pl.ds(i * lanes + n, 1), :] = raw[pl.ds(row, 1), :]
            if hook is not None:
                pl.when(i == 0)(lambda: forward(hook))
            return peak, total

        start = (jnp.full((8, wide), LOW, jnp.float32), jnp.zeros((8, wide), jnp.float32))
        return lax.fori_loop(0, 2, step, start)

    def finish(number, unit, local, peak, total):
        best = jnp.max(peak, axis=0, keepdims=True)
        total = jnp.sum(total * jnp.exp2(peak - best), axis=0, keepdims=True)
        for n in range(2):
            pair = unit[2 * n:2 * n + 2]
            rows_at = slice(n * lanes, (n + 1) * lanes)
            embs = quarters(values_of(pair), inv_e[rows_at, :])
            picked = picks[rows_at, :]
            inv = lax.rsqrt(jnp.sum(picked * picked, axis=1, keepdims=True) + 1e-06)
            picked = quarters(picked, inv)
            cosine = row_sum([u * p for u, p in zip(embs, picked)])
            across = [u - cosine * p for u, p in zip(embs, picked)]
            sine = jnp.sqrt(row_sum([v * v for v in across]))
            target = flip(cosine * COS_MARGIN - sine * SIN_MARGIN)[0:1, :]
            mine = local[:, rows_at]
            owned = (mine >= 0) & (mine < rows)
            tile = 2 * number + n
            stats[tile, 0:1, :] = best[:, rows_at]
            stats[tile, 1:2, :] = total[:, rows_at]
            stats[tile, 2:3, :] = jnp.where(owned, row_of(scale_ref, pair) * target, 0.0)

    def report(number, unit):
        for n, spot in enumerate(unit):
            _, block, p = where_of(spot)

            @pl.loop(0, piece // share)
            def _(t, tile=2 * number + n // 2, start=block * ncls + p * (piece // share)):
                to = start + t

                @pl.when(to != me)
                def _():
                    pltpu.make_async_remote_copy(
                        src_ref=stats.at[tile], dst_ref=got.at[me], send_sem=ss, recv_sem=sr,
                        device_id=(to // ncls, lax.rem(to, ncls)), device_id_type=MESH,
                    ).start()

    stats[:, 3:4, :] = jnp.zeros((2 * len(units), 1, lanes), jnp.float32)
    arrived = 0
    for number, unit in enumerate(units):
        while number >= 2 and arrived < 4 * (number - 1):
            d_copy(arrived).wait_recv()
            arrived += 1
        load_unit(unit)
        local = jnp.concatenate([row_of(lab_ref, unit[0:2]), row_of(lab_ref, unit[2:4])], axis=1) - offset
        below = local - ids
        carry = sweep(unit, below, number if 1 <= number <= 6 else None)
        if number == 0:
            forward(0)
        finish(number, unit, local, *carry)
        if number < 3:
            hear(number + 1)
        elif number == 3:
            for r in range(4, last_round + 1):
                hear(r)
            for k in range(4):
                report(k, units[k])
        else:
            report(number, unit)

    got[me] = stats[2 + lax.rem(cls * share // piece, 4) // 2]
    for copy, plan in ((x_copy, x_plan), (y_copy, y_plan), (z_copy, z_plan), (d_copy, d_order)):
        for k in range(len(plan)):
            copy(k).wait_send()
    rest = got.at[pl.ds(0, ndev - 1)]
    pltpu.make_async_copy(rest, rest, ss).wait()
    pltpu.make_async_copy(rest, rest, sr).wait()

    peaks, totals = got[:, 0, :], got[:, 1, :]
    target = jnp.sum(got[:, 2, :], axis=0, keepdims=True)
    best = jnp.maximum(jnp.max(peaks, axis=0, keepdims=True), target * LOG2E)
    total = jnp.sum(totals * jnp.exp2(peaks - best), axis=0, keepdims=True) + jnp.exp2(target * LOG2E - best)
    loss = best * LN2 + jnp.log(total) - target
    per = lanes // share
    mine = loss[:, 0:share]
    for q in range(1, per):
        mine = jnp.where(lax.rem(me, per) == q, loss[:, q * share:(q + 1) * share], mine)
    out_ref[...] = mine


def body(embeddings, classifier, labels, row_scale):
    ndp, ncls = lax.axis_size("dp"), lax.axis_size("cls")
    assert ndp == 4 and ncls % 4 == 0
    ndev = ndp * ncls
    block, width = embeddings.shape
    rows = classifier.shape[0]
    count = labels.shape[0]
    lanes = block // 4
    chunk = rows // 8
    groups = count // lanes
    f32 = jnp.float32
    any_spec = pl.BlockSpec(memory_space=pl.ANY)
    vmem = pl.BlockSpec(memory_space=pltpu.VMEM)
    dma = pltpu.SemaphoreType.DMA
    out = pl.pallas_call(
        functools.partial(kernel, ndp, ncls, chunk),
        out_shape=jax.ShapeDtypeStruct((1, count // ndev), f32),
        in_specs=[any_spec, any_spec, pl.BlockSpec(memory_space=pltpu.SMEM), vmem, vmem],
        out_specs=vmem,
        scratch_shapes=[
            pltpu.VMEM((4, block, width), f32),
            pltpu.VMEM((rows, width), f32),
            pltpu.VMEM((rows, width), jnp.bfloat16),
            pltpu.VMEM((2 * lanes, width), f32),
            pltpu.VMEM((2 * lanes, width), jnp.bfloat16),
            pltpu.VMEM((2 * lanes, lanes), f32),
            pltpu.VMEM((16, 4, lanes), f32),
            pltpu.VMEM((ndev, 4, lanes), f32),
            dma, dma((8,)), dma((9,)), dma((9,)), dma((9,)), dma((9,)), dma((6,)), dma((6,)),
            dma((24,)), dma((24,)), dma, dma, pltpu.SemaphoreType.REGULAR((ncls // 2 + 1,)),
        ],
        compiler_params=pltpu.CompilerParams(
            collective_id=0, has_side_effects=True, vmem_limit_bytes=56 * 1024 * 1024
        ),
    )(embeddings, classifier, labels, labels.reshape(groups, lanes), row_scale.reshape(groups, lanes))
    return out.reshape(count // ndev)


def solution(mesh):
    placed = (P("dp", None), P(("dp", "cls"), None), P(), P())
    return jax.shard_map(
        body, mesh=mesh, in_specs=placed, out_specs=P(("dp", "cls")), check_vma=False
    )
```

```python
import functools
import math

import jax
import jax.numpy as jnp
from jax import lax
from jax.experimental import pallas as pl
from jax.experimental.pallas import tpu as pltpu
from jax.sharding import PartitionSpec as P

MARGIN = 0.5
COS_MARGIN = math.cos(MARGIN)
SIN_MARGIN = math.sin(MARGIN)
LOG2E = math.log2(math.e)
LN2 = math.log(2.0)
LOW = -1e30
MESH = pl.DeviceIdType.MESH
F, N = 0, 1


def tree(parts, op):
    while len(parts) > 1:
        parts = [op(*parts[k:k + 2]) if k + 1 < len(parts) else parts[k] for k in range(0, len(parts), 2)]
    return parts[0]


def kernel(ndp, ncls, chunk, emb_hbm, cls_hbm, lab_sm, lab_ref, scale_ref, out_ref,
           emb, raw, unit_w, picks, unit_e, inv_e, stats, got,
           emb_sem, raw_sem, xs, xr, ys, yr, zs, zr, ds, dr, ss, sr, rounds):
    dp, cls = lax.axis_index("dp"), lax.axis_index("cls")
    core = lax.rem(cls, 2)
    ndev = ndp * ncls
    me = dp * ncls + cls
    rows, width = cls_hbm.shape
    piece = emb_hbm.shape[0] // 8
    part = piece // 2
    groups, lanes = lab_ref.shape
    nchunk = rows // chunk
    offset = me * rows
    share = groups * lanes // ndev

    emb_in = pltpu.make_async_copy(emb_hbm, emb.at[0], emb_sem)
    emb_in.start()
    to_x = (dp ^ 1, cls)
    to_y = (dp ^ 2, cls)
    to_z = (dp, cls ^ 2)
    partner = (dp, cls ^ 1)
    has_low, has_high = cls >= 2, cls + 2 < ncls
    beside = 3 + has_low.astype(jnp.int32) + has_high.astype(jnp.int32)

    def greet(sem):
        for to in (to_x, to_y, partner):
            pl.semaphore_signal(sem, inc=1, device_id=to, device_id_type=MESH)

        @pl.when(has_low)
        def _():
            pl.semaphore_signal(sem, inc=1, device_id=(dp, cls - 2), device_id_type=MESH)

        @pl.when(has_high)
        def _():
            pl.semaphore_signal(sem, inc=1, device_id=(dp, cls + 2), device_id_type=MESH)

    barrier = pltpu.get_barrier_semaphore()
    greet(barrier)

    raw_in = [
        pltpu.make_async_copy(cls_hbm.at[pl.ds(i * chunk, chunk)], raw.at[pl.ds(i * chunk, chunk)], raw_sem.at[i])
        for i in range(nchunk)
    ]
    for copy in raw_in:
        copy.start()
    emb_in.wait()
    pl.semaphore_wait(barrier, beside)
    last_round = ncls // 2
    greet(rounds.at[0])

    def hear(r):
        pl.semaphore_wait(rounds.at[r], beside)
        if r < last_round:
            greet(rounds.at[r + 1])

    near = cls * share // (4 * piece) * 4
    starts = (4 - near, near)
    turn = lax.rem(cls // 2, 2) * 2
    sx = (0, turn)
    sy = (2, -turn)

    def place(half, index):
        base, shift = index
        return starts[half] + base + shift

    def at(index, by):
        return (index[0] + by, index[1])

    def own(slot, p):
        return emb.at[slot, pl.ds(p * piece + core * part, part)]

    def send(source, slot, p, s, r, k, to):
        copy = pltpu.make_async_remote_copy(
            src_ref=own(source, p), dst_ref=own(slot, p), send_sem=s.at[k], recv_sem=r.at[k],
            device_id=to, device_id_type=MESH,
        )
        copy.start()
        return copy

    x_plan = [(1, F, sx), (1, F, at(sx, 1)), (1, N, sx), (1, N, at(sx, 1)), (3, F, sy), (3, F, at(sy, 1)),
              (1, N, at(sy, 1)), (3, N, sy), (3, N, at(sy, 1))]
    y_plan = [(2, F, at(sy, 1)), (2, F, sy), (2, N, at(sy, 1)), (2, N, sy), (3, F, at(sx, 1)), (3, F, sx),
              (2, N, sx), (3, N, at(sx, 1)), (3, N, sx)]
    z_plan = [(1, F, sx), (2, F, at(sy, 1)), (1, F, at(sx, 1)), (2, F, sy), (1, N, sx), (2, N, at(sy, 1))]

    def other(index):
        return (2 - index[0] if index[0] % 2 == 0 else 4 - index[0], -index[1])

    came_z = [(slot, half, other(index)) for slot, half, index in z_plan]

    def remote(spot, source, s, r, k, to):
        slot, half, index = spot
        p = place(half, index)
        return pltpu.make_async_remote_copy(
            src_ref=own(source, p), dst_ref=own(slot, p), send_sem=s.at[k], recv_sem=r.at[k],
            device_id=to, device_id_type=MESH,
        )

    def x_copy(k):
        return remote(x_plan[k], 0 if x_plan[k][0] == 1 else 2, xs, xr, k, to_x)

    def y_copy(k):
        return remote(y_plan[k], 0 if y_plan[k][0] == 2 else 1, ys, yr, k, to_y)

    def z_copy(k):
        return remote(z_plan[k], z_plan[k][0], zs, zr, k, to_z)

    def d_copy(k):
        copy, plan, n = d_order[k]
        return remote(plan[n], plan[n][0], ds, dr, k, partner)

    X, Y, Z = (x_copy, x_plan), (y_copy, y_plan), (z_copy, came_z)
    arrivals = [
        [(*X, 0), (*Y, 0)],
        [(*X, 1), (*Y, 1)],
        [(*X, 2), (*Y, 2), (*X, 3), (*Y, 3)],
        [(*Z, 0), (*Z, 1), (*X, 4), (*Y, 4)],
        [(*Z, 2), (*X, 5), (*Y, 5), (*Z, 3)],
        [(*X, 6), (*Y, 6), (*Z, 4), (*Y, 7)],
        [(*X, 7), (*X, 8), (*Y, 8), (*Z, 5)],
    ]
    relays = [
        [(z_copy, 0), (z_copy, 1)],
        [(x_copy, 4), (y_copy, 4), (z_copy, 2), (z_copy, 3), (x_copy, 5), (y_copy, 5), (x_copy, 6), (y_copy, 6)],
        [(z_copy, 4), (z_copy, 5), (x_copy, 7), (y_copy, 7), (x_copy, 8), (y_copy, 8)],
        [], [], [], [],
    ]
    d_order = [entry for step in arrivals for entry in step]

    def forward(step):
        done = sum(len(group) for group in arrivals[:step])
        for n, (copy, _, k) in enumerate(arrivals[step]):
            copy(k).wait_recv()
            d_copy(done + n).start()
        for copy, k in relays[step]:
            copy(k).start()

    for k in range(4):
        x_copy(k).start()
        y_copy(k).start()

    def prepare(i):
        raw_in[i].wait()

        @pl.loop(0, chunk // 256)
        def _(b):
            rows_at = pl.ds(pl.multiple_of(i * chunk + b * 256, 256), 256)
            w = raw[rows_at, :]
            inv = lax.rsqrt(jnp.sum(w * w, axis=1, keepdims=True) + 1e-06)
            unit_w[rows_at, :] = (w * inv).astype(jnp.bfloat16)

    for i in range(nchunk):
        prepare(i)
    hear(0)

    zx, zy = sy, sx
    units = [
        [(0, F, (0, 0)), (0, F, (1, 0)), (0, F, (2, 0)), (0, F, (3, 0))],
        [(0, N, (0, 0)), (0, N, (1, 0)), (0, N, (2, 0)), (0, N, (3, 0))],
        [(1, F, sx), (1, F, at(sx, 1)), (2, F, sy), (2, F, at(sy, 1))],
        [(1, N, sx), (1, N, at(sx, 1)), (2, N, sy), (2, N, at(sy, 1))],
        [(1, F, zx), (2, F, at(zy, 1)), (3, F, sy), (3, F, at(sx, 1))],
        [(3, F, sx), (3, F, at(sy, 1)), (2, F, zy), (1, F, at(zx, 1))],
        [(2, N, sx), (1, N, at(sy, 1)), (1, N, zx), (3, N, at(sx, 1))],
        [(3, N, sy), (3, N, at(sy, 1)), (3, N, sx), (2, N, at(zy, 1))],
    ]
    wide = 4 * piece
    tall = rows // 2
    group_rows = 64
    ids = lax.broadcasted_iota(jnp.int32, (8, wide), 0)
    first_half = lax.broadcasted_iota(jnp.int32, (1, lanes), 1) < piece

    def where_of(spot):
        slot, half, index = spot
        return slot, dp ^ slot, place(half, index)

    def row_of(ref, pair):
        both = []
        for spot in pair:
            _, block, p = where_of(spot)
            both.append(ref[pl.ds(block * 4 + p // 2, 1), :])
        return jnp.where(first_half, both[0], both[1])

    def values_of(pair):
        both = []
        for spot in pair:
            slot, _, p = where_of(spot)
            both.append(emb[slot, pl.ds(pl.multiple_of(p * piece, piece), piece), :])
        return jnp.concatenate(both, axis=0) if len(both) > 1 else both[0]

    def quarters(values, factor):
        return [values[:, q:q + lanes] if factor is None else values[:, q:q + lanes] * factor for q in range(0, width, lanes)]

    def row_sum(parts):
        return jnp.sum(tree(parts, jnp.add), axis=1, keepdims=True)

    def flip(values):
        return jnp.transpose(jnp.broadcast_to(values, (lanes, lanes)))

    def load_unit(unit):
        for n in range(2):
            pair = unit[2 * n:2 * n + 2]
            values = values_of(pair)
            inv = lax.rsqrt(jnp.sum(values * values, axis=1, keepdims=True) + 1e-06)
            rows_at = slice(n * lanes, (n + 1) * lanes)
            inv_e[rows_at, :] = jnp.broadcast_to(inv, (lanes, lanes))
            factor = flip(row_of(scale_ref, pair) * LOG2E) * inv
            unit_e[rows_at, :] = jnp.concatenate(
                [v.astype(jnp.bfloat16) for v in quarters(values, factor)], axis=1)

    def sweep(unit, below, hook):
        bases = []
        for spot in unit:
            _, block, p = where_of(spot)
            bases.append((block * 8 + p) * piece)
        count = lanes * group_rows // tall

        def step(i, carry):
            peak, total = carry
            logits = lax.dot_general(
                unit_w[pl.ds(pl.multiple_of(i * tall, tall), tall), :], unit_e[...], (((1,), (1,)), ((), ())),
                preferred_element_type=jnp.float32,
            )
            here = below - i * tall
            base = [jnp.where(i == 0, bases[k], bases[2 + k]) for k in range(2)]
            for g in range(0, tall, group_rows):
                z = [jnp.where(here == r, LOW, logits[r:r + 8, :]) for r in range(g, g + group_rows, 8)]
                fresh = jnp.maximum(peak, tree(z, jnp.maximum))
                terms = [jnp.exp2(t - fresh) for t in z] + [total * jnp.exp2(peak - fresh)]
                peak, total = fresh, tree(terms, jnp.add)
                t = g // group_rows * count
                for n in range(t, t + count):
                    label = lab_sm[base[n // piece] + n % piece]
                    row = lax.rem(label, rows) if rows & (rows - 1) else label & (rows - 1)
                    picks[pl.ds(i * lanes + n, 1), :] = raw[pl.ds(row, 1), :]
            if hook is not None:
                pl.when(i == 0)(lambda: forward(hook))
            return peak, total

        start = (jnp.full((8, wide), LOW, jnp.float32), jnp.zeros((8, wide), jnp.float32))
        return lax.fori_loop(0, 2, step, start)

    def finish(number, unit, local, peak, total):
        best = jnp.max(peak, axis=0, keepdims=True)
        total = jnp.sum(total * jnp.exp2(peak - best), axis=0, keepdims=True)
        for n in range(2):
            pair = unit[2 * n:2 * n + 2]
            rows_at = slice(n * lanes, (n + 1) * lanes)
            columns = []
            for h, spot in enumerate(pair):
                part_at = slice(n * lanes + h * piece, n * lanes + (h + 1) * piece)
                embs = quarters(values_of([spot]), inv_e[part_at, :])
                picked = picks[part_at, :]
                inv = lax.rsqrt(row_sum([v * v for v in quarters(picked, None)]) + 1e-06)
                picked = quarters(picked, inv)
                cosine = row_sum([u * p for u, p in zip(embs, picked)])
                across = [u - cosine * p for u, p in zip(embs, picked)]
                sine = jnp.sqrt(row_sum([v * v for v in across]))
                columns.append(jnp.broadcast_to(cosine * COS_MARGIN - sine * SIN_MARGIN, (piece, lanes)))
            target = jnp.transpose(jnp.concatenate(columns, axis=0))[0:1, :]
            mine = local[:, rows_at]
            owned = (mine >= 0) & (mine < rows)
            tile = 2 * number + n
            stats[tile, 0:1, :] = best[:, rows_at]
            stats[tile, 1:2, :] = total[:, rows_at]
            stats[tile, 2:3, :] = jnp.where(owned, row_of(scale_ref, pair) * target, 0.0)

    def report(number, unit):
        for n, spot in enumerate(unit):
            _, block, p = where_of(spot)

            @pl.loop(0, piece // share)
            def _(t, tile=2 * number + n // 2, start=block * ncls + p * (piece // share)):
                to = start + t

                @pl.when(to != me)
                def _():
                    pltpu.make_async_remote_copy(
                        src_ref=stats.at[tile], dst_ref=got.at[me], send_sem=ss, recv_sem=sr,
                        device_id=(to // ncls, lax.rem(to, ncls)), device_id_type=MESH,
                    ).start()

    stats[:, 3:4, :] = jnp.zeros((2 * len(units), 1, lanes), jnp.float32)
    arrived = 0
    for number, unit in enumerate(units):
        while number >= 2 and arrived < 4 * (number - 1):
            d_copy(arrived).wait_recv()
            arrived += 1
        load_unit(unit)
        local = jnp.concatenate([row_of(lab_ref, unit[0:2]), row_of(lab_ref, unit[2:4])], axis=1) - offset
        below = local - ids
        carry = sweep(unit, below, number if 1 <= number <= 6 else None)
        if number == 0:
            forward(0)
        finish(number, unit, local, *carry)
        if number < 3:
            hear(number + 1)
        elif number == 3:
            for r in range(4, last_round + 1):
                hear(r)
            for k in range(4):
                report(k, units[k])
        else:
            report(number, unit)

    got[me] = stats[2 + lax.rem(cls * share // piece, 4) // 2]
    for copy, plan in ((x_copy, x_plan), (y_copy, y_plan), (z_copy, z_plan), (d_copy, d_order)):
        for k in range(len(plan)):
            copy(k).wait_send()
    rest = got.at[pl.ds(0, ndev - 1)]
    pltpu.make_async_copy(rest, rest, ss).wait()
    pltpu.make_async_copy(rest, rest, sr).wait()

    peaks, totals = got[:, 0, :], got[:, 1, :]
    target = jnp.sum(got[:, 2, :], axis=0, keepdims=True)
    best = jnp.maximum(jnp.max(peaks, axis=0, keepdims=True), target * LOG2E)
    total = jnp.sum(totals * jnp.exp2(peaks - best), axis=0, keepdims=True) + jnp.exp2(target * LOG2E - best)
    loss = best * LN2 + jnp.log(total) - target
    per = lanes // share
    mine = loss[:, 0:share]
    for q in range(1, per):
        mine = jnp.where(lax.rem(me, per) == q, loss[:, q * share:(q + 1) * share], mine)
    out_ref[...] = mine


def body(embeddings, classifier, labels, row_scale):
    ndp, ncls = lax.axis_size("dp"), lax.axis_size("cls")
    assert ndp == 4 and ncls % 4 == 0
    ndev = ndp * ncls
    block, width = embeddings.shape
    rows = classifier.shape[0]
    count = labels.shape[0]
    lanes = block // 4
    chunk = rows // 8
    groups = count // lanes
    f32 = jnp.float32
    any_spec = pl.BlockSpec(memory_space=pl.ANY)
    vmem = pl.BlockSpec(memory_space=pltpu.VMEM)
    dma = pltpu.SemaphoreType.DMA
    out = pl.pallas_call(
        functools.partial(kernel, ndp, ncls, chunk),
        out_shape=jax.ShapeDtypeStruct((1, count // ndev), f32),
        in_specs=[any_spec, any_spec, pl.BlockSpec(memory_space=pltpu.SMEM), vmem, vmem],
        out_specs=vmem,
        scratch_shapes=[
            pltpu.VMEM((4, block, width), f32),
            pltpu.VMEM((rows, width), f32),
            pltpu.VMEM((rows, width), jnp.bfloat16),
            pltpu.VMEM((2 * lanes, width), f32),
            pltpu.VMEM((2 * lanes, width), jnp.bfloat16),
            pltpu.VMEM((2 * lanes, lanes), f32),
            pltpu.VMEM((16, 4, lanes), f32),
            pltpu.VMEM((ndev, 4, lanes), f32),
            dma, dma((8,)), dma((9,)), dma((9,)), dma((9,)), dma((9,)), dma((6,)), dma((6,)),
            dma((24,)), dma((24,)), dma, dma, pltpu.SemaphoreType.REGULAR((ncls // 2 + 1,)),
        ],
        compiler_params=pltpu.CompilerParams(
            collective_id=0, has_side_effects=True, vmem_limit_bytes=56 * 1024 * 1024
        ),
    )(embeddings, classifier, labels, labels.reshape(groups, lanes), row_scale.reshape(groups, lanes))
    return out.reshape(count // ndev)


def solution(mesh):
    placed = (P("dp", None), P(("dp", "cls"), None), P(), P())
    return jax.shard_map(
        body, mesh=mesh, in_specs=placed, out_specs=P(("dp", "cls")), check_vma=False
    )
```
